128 devices in a mesh: seq: 32 (over x, z, core), head: 4 (over y).
Axes of the slice: x: 4, y: 4, z: 4, core: 2. Of those that a mesh axis runs over, the one named last changes fastest.
Arguments:
- queries: bfloat16 [4, 4, 4, 32, 128], P(None, None, 'head', 'seq'), may hold values from -512 to 512
- key_codes: bfloat16 [4, 8, 8192, 16, 128], P(None, 'head', 'seq'), may hold values from -8 to 7, as said below
- value_codes: bfloat16 [4, 8, 8192, 16, 128], P(None, 'head', 'seq'), may hold values from -8 to 7, as said below
- key_scales: float32 [4, 8, 8192], P(None, 'head', 'seq'), may hold values from 0.05 to 0.5
- value_scales: float32 [4, 8, 8192], P(None, 'head', 'seq'), may hold values from 0.05 to 0.5
- page_ids: int32 [4, 4, 8, 4096], P(None, None, 'head', 'seq'), may hold values from 0 to 8191, as said below
- page_counts: int32 [4, 4, 8, 32], P(None, None, 'head', 'seq'), may hold values from 0 to 128, as said below
- out_weight: bfloat16 [16384, 16384], P('head', 'seq'), may hold values from -0.046875 to 0.046875
Outputs:
- projected: bfloat16 [4, 4, 16384], P(None, None, ('seq', 'head'))
The draws below stay inside these ranges and needn't reach their ends.
Inputs may be any that keep to these rules, and one draw needn't show every extreme that they name: `page_ids`: slots r * 128 to (r + 1) * 128 - 1 name distinct pages of range r, that is pages r * 256 to (r + 1) * 256 - 1. `page_counts`: in every row of 32 counts some range has all 128 slots valid. `key_codes`: whole numbers. `value_codes`: whole numbers.
All inputs are finite; a program needn't handle non-finite values.
Results may differ from the reference program's by a relative error of at most 0.012.
The reference program's roundings to bfloat16 on the way (of `rounded` and `attended`) count: a program that leaves them out, or rounds other values in their place, can miss the bound.
Values may be sent and summed in bfloat16 or wider, within the bound.
A program may use at most 128 MiB of HBM per device.

```python
import math
import jax
import jax.numpy as jnp
from jax import lax

D = 16384
HEADS = 128
KVH = 8
HD = 128
PAGE = 16
STEPS = 4
SEQS = 4
PAGES_DEV = 256
SLOTS = 128
POSITION_SPANS = 32
NPAGES = 8192
GROUP = 32
GROUPS = 4


def code_table(key, salt):
    raw = jax.random.randint(jax.random.fold_in(key, salt), (SEQS, KVH, NPAGES, PAGE, HD), -8, 8)
    return raw.astype(jnp.float32)


def scale_table(key, salt, lowest):
    spread = jax.random.uniform(jax.random.fold_in(key, salt), (SEQS, KVH, NPAGES), jnp.float32, math.log(lowest), math.log(0.5))
    return jnp.exp(spread)


def count_table(key):
    ceiling = jax.random.randint(jax.random.fold_in(key, 31), (1, 1, KVH, POSITION_SPANS), 0, SLOTS + 1)
    base = jax.random.randint(jax.random.fold_in(key, 37), (STEPS, SEQS, KVH, POSITION_SPANS), 0, ceiling + 1)
    hottest = jax.random.randint(jax.random.fold_in(key, 41), (STEPS, SEQS, KVH, 1), 0, POSITION_SPANS)
    place = lax.broadcasted_iota(jnp.int32, (STEPS, SEQS, KVH, POSITION_SPANS), 3)
    return jnp.where(place == hottest, SLOTS, base).astype(jnp.int32)


def id_table(key):
    random_bits = jax.random.randint(jax.random.fold_in(key, 47), (STEPS, SEQS, KVH, POSITION_SPANS, PAGES_DEV), 0, 1 << 20)
    ranked = random_bits * PAGES_DEV + lax.broadcasted_iota(jnp.int32, (STEPS, SEQS, KVH, POSITION_SPANS, PAGES_DEV), 4)
    order = jnp.argsort(ranked, axis=-1)
    offsets = lax.broadcasted_iota(jnp.int32, (STEPS, SEQS, KVH, POSITION_SPANS, SLOTS), 3) * PAGES_DEV
    chosen_ids = order[..., :SLOTS].astype(jnp.int32) + offsets
    return chosen_ids.reshape(STEPS, SEQS, KVH, POSITION_SPANS * SLOTS)


def draw_page_ids(key, part):
    return id_table(key)


def draw_page_counts(key, part):
    return count_table(key)


def draw_key_codes(key, part):
    return code_table(key, 17).astype(jnp.bfloat16)


def draw_value_codes(key, part):
    return code_table(key, 19).astype(jnp.bfloat16)


def draw_key_scales(key, part):
    return scale_table(key, 23, 0.05)


def draw_value_scales(key, part):
    return scale_table(key, 29, 0.05)


def draw_queries(key, part):
    shape = (STEPS, SEQS, HEADS, HD)
    whole = jax.random.normal(jax.random.fold_in(key, 5), shape, jnp.float32)
    return whole.reshape(STEPS, SEQS, GROUPS, GROUP, HD).astype(jnp.bfloat16)


def steps_of(stream_key, shape, pieces, least, high):
    level = 1.0
    for position, blocks in pieces:
        steps = jax.random.uniform(jax.random.fold_in(jax.random.fold_in(stream_key, 6), position), (blocks,), jnp.float32, least / len(pieces), high / len(pieces))
        level = level * jnp.repeat(jnp.exp(steps), shape[position] // blocks).reshape((-1,) + (1,) * (len(shape) - 1 - position))
    return level


def centred(own_key, shape, deviation, bound, pieces=(), held_as=jnp.bfloat16):
    entries = deviation * jax.random.normal(own_key, shape, jnp.float32)
    if pieces:
        entries = entries * steps_of(own_key, shape, pieces, -0.22, 0.18)
    return jnp.clip(entries, -bound, bound).astype(held_as)


def setup_inputs(seed: int = 0) -> dict:
    seeds = jax.random.split(jax.random.key(seed), 9)
    queries = draw_queries(jax.random.fold_in(seeds[8], 71), 0)
    key_codes = draw_key_codes(jax.random.fold_in(seeds[8], 71), 0)
    value_codes = draw_value_codes(jax.random.fold_in(seeds[8], 71), 0)
    key_scales = draw_key_scales(jax.random.fold_in(seeds[8], 71), 0)
    value_scales = draw_value_scales(jax.random.fold_in(seeds[8], 71), 0)
    page_ids = draw_page_ids(jax.random.fold_in(seeds[8], 71), 0)
    page_counts = draw_page_counts(jax.random.fold_in(seeds[8], 71), 0)
    out_weight = centred(seeds[7], (HEADS * HD, D), (HEADS * HD) ** -0.5, 0.046875, ((0, 4), (1, 32)))
    return {"queries": queries, "key_codes": key_codes, "value_codes": value_codes, "key_scales": key_scales, "value_scales": value_scales, "page_ids": page_ids, "page_counts": page_counts, "out_weight": out_weight}


NEG_FILL = -1e+30

def reference(queries, key_codes, value_codes, key_scales, value_scales, page_ids, page_counts, out_weight):
    queries_per_key_head = HEADS // KVH
    query_blocks = queries.reshape(STEPS, SEQS, KVH, queries_per_key_head, HD)
    inverse_sqrt_scale = 1.0 / math.sqrt(HD)
    slot_line = jnp.arange(SLOTS, dtype=jnp.int32)

    def pick_head(table, step_index, head_index):
        return lax.dynamic_index_in_dim(lax.dynamic_index_in_dim(table, step_index, 0, False), head_index, 1, False)

    def attend(flat_index):
        step_index = flat_index // KVH
        head_index = flat_index % KVH
        current_query = pick_head(query_blocks, step_index, head_index)
        ids_now = pick_head(page_ids, step_index, head_index).astype(jnp.int32)
        counts_now = pick_head(page_counts, step_index, head_index)
        key_table = lax.dynamic_index_in_dim(key_codes, head_index, 1, False)
        value_table = lax.dynamic_index_in_dim(value_codes, head_index, 1, False)
        key_factor = jnp.take_along_axis(lax.dynamic_index_in_dim(key_scales, head_index, 1, False), ids_now, axis=1)
        value_factor = jnp.take_along_axis(lax.dynamic_index_in_dim(value_scales, head_index, 1, False), ids_now, axis=1)
        index_wide = jnp.broadcast_to(ids_now[:, :, None, None], (SEQS, POSITION_SPANS * SLOTS, PAGE, HD))
        key_picked = jnp.take_along_axis(key_table, index_wide, axis=1)
        value_picked = jnp.take_along_axis(value_table, index_wide, axis=1)
        key_row_block = (key_picked.astype(jnp.float32) * key_factor[:, :, None, None]).astype(jnp.bfloat16)
        value_rows = (value_picked.astype(jnp.float32) * value_factor[:, :, None, None]).astype(jnp.bfloat16)
        key_row_block = key_row_block.reshape(SEQS, POSITION_SPANS, SLOTS * PAGE, HD).astype(jnp.float32)
        value_rows = value_rows.reshape(SEQS, POSITION_SPANS, SLOTS * PAGE, HD).astype(jnp.float32)
        logit_scores = jnp.einsum('keo,kulo->keul', current_query.astype(jnp.float32), key_row_block, precision=lax.Precision.HIGHEST) * inverse_sqrt_scale
        live_slots = slot_line[None, None, :] < counts_now[:, :, None]
        chosen = jnp.repeat(live_slots, PAGE, axis=2)[:, None, :, :]
        masked = jnp.where(chosen, logit_scores, NEG_FILL)
        peak_score = lax.optimization_barrier(jnp.max(masked, axis=-1))
        weights = jnp.where(chosen, jnp.exp(masked - peak_score[..., None]), 0.0)
        weight_total = lax.optimization_barrier(jnp.sum(weights, axis=-1))
        rounded = weights.astype(jnp.bfloat16)
        partial_value = jnp.einsum('bqrn,brnd->bqrd', rounded.astype(jnp.float32), value_rows, precision=lax.Precision.HIGHEST)
        top_score = lax.optimization_barrier(jnp.max(peak_score, axis=2))
        factor = jnp.exp(peak_score - top_score[..., None])
        total_all = lax.optimization_barrier(jnp.sum(factor * weight_total, axis=2))
        summed = lax.optimization_barrier(jnp.sum(factor[..., None] * partial_value, axis=2))
        return (summed / total_all[..., None]).astype(jnp.bfloat16)
    attended = lax.map(attend, jnp.arange(STEPS * KVH, dtype=jnp.int32))
    attended = attended.reshape(STEPS, KVH, SEQS, queries_per_key_head, HD).transpose(0, 2, 1, 3, 4)
    attended = attended.reshape(STEPS * SEQS, HEADS * HD)
    projected = jnp.dot(attended, out_weight, preferred_element_type=jnp.float32).astype(jnp.bfloat16)
    return projected.reshape(STEPS, SEQS, D)
```

```python
import functools
import math

import jax
import jax.numpy as jnp
from jax import lax
from jax.experimental import pallas as pl
from jax.experimental.pallas import tpu as pltpu
from jax.sharding import PartitionSpec as P

MESH = pl.DeviceIdType.MESH
F32 = jnp.float32
BF16 = jnp.bfloat16
CHUNK = 256
PART = 4


def seq_offsets(count):
    parts = (4, 4, 2) if count == 32 else (1, 1, count)
    steps = [(i, j, k) for i in range(parts[0]) for j in range(parts[1]) for k in range(parts[2])]
    ring = lambda d, n: min(d, n - d)
    steps = sorted(steps, key=lambda o: -(4 * (ring(o[0], parts[0]) + ring(o[1], parts[1])) + o[2]))
    return parts, steps[:-1]


def seq_peers(me, count):
    parts, steps = seq_offsets(count)
    x, z, core = me // (parts[1] * parts[2]), (me // parts[2]) % parts[1], me % parts[2]
    xs = [((x + d) % parts[0]) * (parts[1] * parts[2]) for d in range(parts[0])]
    zs = [((z + d) % parts[1]) * parts[2] for d in range(parts[1])]
    cores = [(core + d) % parts[2] for d in range(parts[2])]
    return [(o, xs[o[0]] + zs[o[1]] + cores[o[2]]) for o in steps], parts, xs


def attend_kernel(
    sizes,
    q_hbm,
    k_hbm,
    v_hbm,
    ks_hbm,
    vs_hbm,
    ids_hbm,
    cnt_hbm,
    w_hbm,
    out_ref,
    k_v,
    v_v,
    w_v,
    ks_v,
    vs_v,
    ids_v,
    cnt_v,
    kt_v,
    idm,
    hits,
    bias,
    q_all,
    q_f32,
    s_buf,
    m_buf,
    o_f32,
    a_buf,
    o_send,
    o_in,
    st_send,
    st_in,
    att_all,
    h_send,
    h_in,
    local_sem,
    k_sem,
    v_sem,
    send_sem,
    recv_sem,
):
    n_seq, n_head, steps, seqs, kvl, pages, page_len, hd = sizes
    group = n_seq
    rows = group * steps
    half = rows // kvl
    positions = pages * page_len
    chunks = positions // CHUNK
    chunk_pages = CHUNK // page_len
    slots = ids_v.shape[3]
    row_count = steps * seqs
    me = lax.axis_index("seq")
    my_head = lax.axis_index("head")
    peers, parts, plane_first = seq_peers(me, n_seq)
    planes = parts[0]
    plane = n_seq // planes

    q_copy = pltpu.make_async_copy(q_hbm, q_all.at[me], local_sem.at[0])
    ids_copy = pltpu.make_async_copy(ids_hbm, ids_v, local_sem.at[1])
    cnt_copy = pltpu.make_async_copy(cnt_hbm, cnt_v, local_sem.at[2])
    ks_copy = pltpu.make_async_copy(ks_hbm, ks_v, local_sem.at[3])
    vs_copy = pltpu.make_async_copy(vs_hbm, vs_v, local_sem.at[4])
    w_copy = pltpu.make_async_copy(w_hbm, w_v, local_sem.at[5])

    def k_copy(b):
        return pltpu.make_async_copy(k_hbm.at[b], k_v.at[b], k_sem.at[b])

    def v_copy(b):
        return pltpu.make_async_copy(v_hbm.at[b], v_v.at[b], v_sem.at[b])

    for copy in (q_copy, ids_copy, cnt_copy, ks_copy, vs_copy):
        copy.start()

    barrier = pltpu.get_barrier_semaphore()

    for _, peer in peers:
        pl.semaphore_signal(barrier, inc=1, device_id={"seq": peer}, device_id_type=MESH)
    for i in range(1, n_head):
        pl.semaphore_signal(
            barrier, inc=1, device_id={"head": (my_head + i) % n_head}, device_id_type=MESH
        )
    for b in range(seqs):
        k_copy(b).start()
        v_copy(b).start()
    w_copy.start()

    def push(src, dst, which, peer, arrival=None):
        pltpu.make_async_remote_copy(
            src_ref=src,
            dst_ref=dst,
            send_sem=send_sem.at[which],
            recv_sem=recv_sem.at[which if arrival is None else arrival],
            device_id={"seq": peer},
            device_id_type=MESH,
        ).start()

    def whole(ref, which, axis, count, arrival=None):
        block = ref.at[pl.ds(0, count)]
        return pltpu.make_async_remote_copy(
            src_ref=block,
            dst_ref=block,
            send_sem=send_sem.at[which],
            recv_sem=recv_sem.at[which if arrival is None else arrival],
            device_id={axis: 0},
            device_id_type=MESH,
        )

    ids_copy.wait()
    cnt_copy.wait()
    first_page = me * pages
    slot_iota = lax.broadcasted_iota(jnp.int32, (kvl, slots), 1)
    for t in range(steps):
        for b in range(seqs):
            counts = [
                jnp.broadcast_to(cnt_v[t, k][:, b : b + 1], (1, slots)) for k in range(kvl)
            ]
            live = slot_iota < jnp.concatenate(counts, axis=0)
            local = jnp.where(live, ids_v[t, b] - first_page, -1)
            idm[pl.ds((t * seqs + b) * kvl, kvl), :] = local.astype(F32)
    by_slot = jnp.transpose(idm[...])
    page_line = lax.broadcasted_iota(jnp.int32, (slots, pages), 1).astype(F32)
    for t in range(steps):
        for b in range(seqs):
            for k in range(kvl):
                r = (t * seqs + b) * kvl + k
                column = jnp.broadcast_to(by_slot[:, r : r + 1], (slots, pages))
                found = jnp.max(jnp.where(column == page_line, 1.0, 0.0), axis=0, keepdims=True)
                for s in range(8 // steps):
                    hits[b * kvl + k, pl.ds(s * steps + t, 1), :] = found

    q_copy.wait()
    pl.semaphore_wait(barrier, n_seq - 1 + n_head - 1)
    for _, peer in peers:
        push(q_all.at[me], q_all.at[me], 0, peer)

    page_of = lax.broadcasted_iota(jnp.int32, (pages, CHUNK), 0) % chunk_pages
    spot_of = lax.broadcasted_iota(jnp.int32, (pages, CHUNK), 1) // page_len
    spread = jnp.where(page_of == spot_of, 1.0, 0.0).astype(BF16)
    chunk_id = lax.broadcasted_iota(jnp.int32, (chunks, 8, pages), 0)
    in_chunk = lax.broadcasted_iota(jnp.int32, (chunks, 8, pages), 2) // chunk_pages == chunk_id

    def expand(entry):
        stacked = jnp.where(in_chunk, jnp.broadcast_to(entry[None], (chunks, 8, pages)), 0.0)
        stacked = stacked.reshape(chunks * 8, pages).astype(BF16)
        return jnp.dot(stacked, spread, preferred_element_type=F32).reshape(chunks, 8, CHUNK)

    log2e = 1.0 / math.log(2.0)
    score_factor = log2e / math.sqrt(hd)

    for bk in range(seqs * kvl):
        bias[bk] = (expand(hits[bk]) - 1.0) * 1e30

    ks_copy.wait()
    vs_copy.wait()

    def scaled(ref, scales, b, k, c):
        lines = []
        for i in range(chunk_pages):
            p = c * chunk_pages + i
            scale = scales[b * (kvl * pages // 128) + (p // 128) * kvl + k, p % 128]
            codes = ref[b, k, pl.ds(p * page_len, page_len), :].astype(F32)
            lines.append((codes * scale).astype(BF16))
        return jnp.concatenate(lines, axis=0)

    @pl.loop(0, seqs)
    def _(b):
        k_copy(b).wait()
        for c in range(chunks):
            for k in range(kvl):
                kt_v[b, c, pl.ds(k * hd, hd), :] = jnp.transpose(scaled(k_v, ks_v, b, k, c))
        v_copy(b).wait()
        for c in range(chunks):
            for k in range(kvl):
                v_v[b, k, pl.ds(c * CHUNK, CHUNK), :] = scaled(v_v, vs_v, b, k, c)

    whole(q_all, 0, "seq", n_seq - 1).wait_recv()
    q_f32[...] = q_all[...].astype(F32).reshape(group * row_count, hd)

    row_line = lax.broadcasted_iota(jnp.int32, (rows, hd), 0)
    lane_line = lax.broadcasted_iota(jnp.int32, (rows, hd), 1)

    def packed_queries(b):
        mine = q_f32[pl.ds(b, rows, stride=seqs), :]
        return jnp.concatenate(
            [jnp.where(row_line // half == k, mine, 0.0) for k in range(kvl)], axis=1
        ).astype(BF16)

    def score_part(b, part, queries, peak):
        for i in range(PART):
            c = part * PART + i
            raw = jnp.dot(queries, kt_v[b, c], preferred_element_type=F32)
            peaks = []
            for k in range(kvl):
                mine = raw[k * half : (k + 1) * half].reshape(half // 8, 8, CHUNK)
                mine = mine * score_factor + bias[b * kvl + k, c][None]
                mine = mine.reshape(half, CHUNK)
                s_buf[b % 2, c, pl.ds(k * half, half), :] = mine
                top = mine[:, :128]
                for j in range(1, CHUNK // 128):
                    top = jnp.maximum(top, mine[:, j * 128 : (j + 1) * 128])
                peaks.append(top)
            peak = jnp.maximum(peak, jnp.concatenate(peaks, axis=0))
        return peak

    def value_part(b, part, total, acc):
        for i in range(PART):
            c = part * PART + i
            off = c * CHUNK
            weights = []
            sums = []
            for k in range(kvl):
                lines = s_buf[b % 2, c, pl.ds(k * half, half), :]
                peak = m_buf[b % 2, pl.ds(k * half, half), :]
                peak = jnp.concatenate([peak] * (CHUNK // 128), axis=1)
                weight = jnp.exp2(lines - peak)
                part_sum = weight[:, :128]
                for j in range(1, CHUNK // 128):
                    part_sum = part_sum + weight[:, j * 128 : (j + 1) * 128]
                sums.append(part_sum)
                weights.append(weight.astype(BF16))
            values = jnp.concatenate([v_v[b, k, pl.ds(off, CHUNK), :] for k in range(kvl)], axis=1)
            total = total + jnp.concatenate(sums, axis=0)
            acc = acc + jnp.dot(
                jnp.concatenate(weights, axis=0), values, preferred_element_type=F32
            )
        return total, acc

    def set_peak(b, peak):
        peak = jnp.max(peak, axis=1, keepdims=True)
        m_buf[b % 2] = jnp.broadcast_to(peak, (rows, 128))

    low = jnp.full((rows, 128), -2e30, F32)
    first = packed_queries(0)
    peak = low
    for part in range(chunks // PART):
        peak = score_part(0, part, first, peak)
    set_peak(0, peak)
    for b in range(seqs):
        if b + 1 < seqs:
            queries = packed_queries(b + 1)

        peak = low
        total = jnp.zeros((rows, 128), F32)
        acc = jnp.zeros((rows, kvl * hd), F32)
        for part in range(chunks // PART):
            if b + 1 < seqs:
                peak = score_part(b + 1, part, queries, peak)
            total, acc = value_part(b, part, total, acc)
        total = jnp.broadcast_to(jnp.sum(total, axis=1, keepdims=True), (rows, 128))
        mine = jnp.concatenate(
            [acc[k * half : (k + 1) * half, k * hd : (k + 1) * hd] for k in range(kvl)], axis=0
        )
        o_f32[pl.ds(b, rows, stride=seqs), :] = mine / total
        level = m_buf[b % 2] + jnp.log(total) * log2e
        here = jnp.where(lane_line == (row_line % steps) * seqs + b, level, 0.0)
        if b == 0:
            a_buf[...] = here
        else:
            a_buf[...] += here
        if b + 1 < seqs:
            set_peak(b + 1, peak)

    stats = a_buf[pl.ds(0, group, stride=steps), :]
    for t in range(1, steps):
        stats = stats + a_buf[pl.ds(t, group, stride=steps), :]
    st_send[...] = stats.reshape(group, 1, 128)
    o_send[...] = o_f32[...].reshape(group, row_count, hd).astype(BF16)
    for _, peer in peers:
        push(st_send.at[peer], st_in.at[me], 1, peer)
        push(o_send.at[peer], o_in.at[me], 2, peer)
    o_in[me] = o_send[me]
    st_in[me] = st_send[me]
    whole(st_in, 1, "seq", n_seq - 1).wait_recv()
    levels = st_in[...].reshape(group, 128)
    share = jnp.exp2(levels - jnp.max(levels, axis=0, keepdims=True))
    share = share / jnp.sum(share, axis=0, keepdims=True)
    by_row = jnp.transpose(share)[:row_count]
    whole(o_in, 2, "seq", n_seq - 1).wait_recv()
    merged = jnp.zeros((row_count, hd), F32)
    for r in range(n_seq):
        merged = merged + by_row[:, r : r + 1] * o_in[r].astype(F32)
    att_all[me] = merged.astype(BF16)
    for step, peer in peers:
        push(att_all.at[me], att_all.at[me], 3, peer, 5 + (planes - step[0]) % planes)

    w_copy.wait()
    partial = None
    for d in sorted(range(planes), key=lambda d: min(d, planes - d)):
        whole(att_all, 3, "seq", plane - (d == 0), 5 + d).wait_recv()
        first_head = plane_first[d]
        flat = jnp.concatenate([att_all[first_head + j] for j in range(plane)], axis=1)
        lines = w_v[pl.ds(pl.multiple_of(first_head * hd, plane * hd), plane * hd), :]
        term = jnp.dot(flat, lines, preferred_element_type=F32)
        partial = term if partial is None else partial + term
    width = partial.shape[1] // n_head
    for h in range(n_head):
        h_send[h] = partial[:, h * width : (h + 1) * width].astype(BF16)
    for i in range(1, n_head):
        peer = (my_head + i) % n_head
        pltpu.make_async_remote_copy(
            src_ref=h_send.at[peer],
            dst_ref=h_in.at[my_head],
            send_sem=send_sem.at[4],
            recv_sem=recv_sem.at[4],
            device_id={"head": peer},
            device_id_type=MESH,
        ).start()
    h_in[my_head] = h_send[my_head]
    for which, ref in ((0, q_all), (1, st_in), (2, o_in), (3, att_all)):
        whole(ref, which, "seq", n_seq - 1).wait_send()
    whole(h_in, 4, "head", n_head - 1).wait_recv()
    whole(h_in, 4, "head", n_head - 1).wait_send()
    summed = h_in[0].astype(F32)
    for h in range(1, n_head):
        summed = summed + h_in[h].astype(F32)
    out_ref[...] = summed.astype(BF16)


def body(
    queries, key_codes, value_codes, key_scales, value_scales, page_ids, page_counts, out_weight,
    *, n_seq, n_head
):
    steps, seqs, _, _, hd = queries.shape
    _, kvl, pages, page_len, _ = key_codes.shape
    row_count = steps * seqs
    group = n_seq
    rows = group * steps
    positions = pages * page_len
    chunks = positions // CHUNK
    columns = out_weight.shape[1]
    slots = page_ids.shape[3]
    width = columns // n_head

    def by_line(scales):
        scales = scales.reshape(seqs, kvl, pages // 128, 128)
        return jnp.transpose(scales, (0, 2, 1, 3)).reshape(-1, 128)

    any_space = pl.BlockSpec(memory_space=pltpu.HBM)
    sizes = (n_seq, n_head, steps, seqs, kvl, pages, page_len, hd)
    out = pl.pallas_call(
        functools.partial(attend_kernel, sizes),
        out_shape=jax.ShapeDtypeStruct((row_count, width), BF16),
        in_specs=[any_space] * 8,
        out_specs=pl.BlockSpec(memory_space=pltpu.VMEM),
        scratch_shapes=[
            pltpu.VMEM((seqs, kvl, positions, hd), BF16),
            pltpu.VMEM((seqs, kvl, positions, hd), BF16),
            pltpu.VMEM(out_weight.shape, BF16),
            pltpu.SMEM((seqs * kvl * pages // 128, 128), F32),
            pltpu.SMEM((seqs * kvl * pages // 128, 128), F32),
            pltpu.VMEM(page_ids.shape, jnp.int32),
            pltpu.VMEM((steps, kvl, 1, seqs), jnp.int32),
            pltpu.VMEM((seqs, chunks, kvl * hd, CHUNK), BF16),
            pltpu.VMEM((steps * seqs * kvl, slots), F32),
            pltpu.VMEM((seqs * kvl, 8, pages), F32),
            pltpu.VMEM((seqs * kvl, chunks, 8, CHUNK), F32),
            pltpu.VMEM((group, row_count, hd), BF16),
            pltpu.VMEM((group * row_count, hd), F32),
            pltpu.VMEM((2, chunks, rows, CHUNK), F32),
            pltpu.VMEM((2, rows, 128), F32),
            pltpu.VMEM((group * row_count, hd), F32),
            pltpu.VMEM((rows, 128), F32),
            pltpu.VMEM((group, row_count, hd), BF16),
            pltpu.VMEM((group, row_count, hd), BF16),
            pltpu.VMEM((group, 1, 128), F32),
            pltpu.VMEM((group, 1, 128), F32),
            pltpu.VMEM((group, row_count, hd), BF16),
            pltpu.VMEM((n_head, row_count, width), BF16),
            pltpu.VMEM((n_head, row_count, width), BF16),
            pltpu.SemaphoreType.DMA((6,)),
            pltpu.SemaphoreType.DMA((seqs,)),
            pltpu.SemaphoreType.DMA((seqs,)),
            pltpu.SemaphoreType.DMA((5,)),
            pltpu.SemaphoreType.DMA((9,)),
        ],
        compiler_params=pltpu.CompilerParams(
            collective_id=0, has_side_effects=True, vmem_limit_bytes=60 * 1024 * 1024
        ),
        name="attend",
    )(
        queries.reshape(row_count, hd),
        key_codes.reshape(seqs, kvl, positions, hd),
        value_codes.reshape(seqs, kvl, positions, hd),
        by_line(key_scales),
        by_line(value_scales),
        page_ids,
        jnp.transpose(page_counts, (0, 2, 3, 1)),
        out_weight,
    )
    return out.reshape(steps, seqs, width)


def solution(mesh):
    placed = (
        P(None, None, "head", "seq", None),
        P(None, "head", "seq", None, None),
        P(None, "head", "seq", None, None),
        P(None, "head", "seq"),
        P(None, "head", "seq"),
        P(None, None, "head", "seq"),
        P(None, None, "head", "seq"),
        P("head", "seq"),
    )
    step = functools.partial(body, n_seq=mesh.shape["seq"], n_head=mesh.shape["head"])
    return jax.shard_map(
        step, mesh=mesh, in_specs=placed, out_specs=P(None, None, ("seq", "head")), check_vma=False
    )
```

```python
import functools
import math

import jax
import jax.numpy as jnp
from jax import lax
from jax.experimental import pallas as pl
from jax.experimental.pallas import tpu as pltpu
from jax.sharding import PartitionSpec as P

MESH = pl.DeviceIdType.MESH
F32 = jnp.float32
BF16 = jnp.bfloat16
CHUNK = 256
PART = 4


def seq_offsets(count):
    parts = (4, 4, 2) if count == 32 else (1, 1, count)
    steps = [(i, j, k) for i in range(parts[0]) for j in range(parts[1]) for k in range(parts[2])]
    ring = lambda d, n: min(d, n - d)
    steps = sorted(steps, key=lambda o: -(4 * (ring(o[0], parts[0]) + ring(o[1], parts[1])) + o[2]))
    return parts, steps[:-1]


def seq_peers(me, count):
    parts, steps = seq_offsets(count)
    x, z, core = me // (parts[1] * parts[2]), (me // parts[2]) % parts[1], me % parts[2]
    xs = [((x + d) % parts[0]) * (parts[1] * parts[2]) for d in range(parts[0])]
    zs = [((z + d) % parts[1]) * parts[2] for d in range(parts[1])]
    cores = [(core + d) % parts[2] for d in range(parts[2])]
    return [(o, xs[o[0]] + zs[o[1]] + cores[o[2]]) for o in steps], parts, xs


def attend_kernel(
    sizes,
    q_hbm,
    k_hbm,
    v_hbm,
    ks_hbm,
    vs_hbm,
    ids_hbm,
    cnt_hbm,
    w_hbm,
    out_ref,
    k_v,
    v_v,
    w_v,
    ks_v,
    vs_v,
    ids_v,
    cnt_v,
    kt_v,
    idm,
    hits,
    bias,
    q_all,
    q_f32,
    s_buf,
    m_buf,
    o_f32,
    a_buf,
    o_send,
    o_in,
    st_send,
    st_in,
    att_all,
    h_send,
    h_in,
    local_sem,
    k_sem,
    v_sem,
    send_sem,
    recv_sem,
):
    n_seq, n_head, steps, seqs, kvl, pages, page_len, hd = sizes
    group = n_seq
    rows = group * steps
    half = rows // kvl
    positions = pages * page_len
    chunks = positions // CHUNK
    chunk_pages = CHUNK // page_len
    slots = ids_v.shape[3]
    row_count = steps * seqs
    me = lax.axis_index("seq")
    my_head = lax.axis_index("head")
    peers, parts, plane_first = seq_peers(me, n_seq)
    planes = parts[0]
    plane = n_seq // planes

    q_copy = pltpu.make_async_copy(q_hbm, q_all.at[me], local_sem.at[0])
    ids_copy = pltpu.make_async_copy(ids_hbm, ids_v, local_sem.at[1])
    cnt_copy = pltpu.make_async_copy(cnt_hbm, cnt_v, local_sem.at[2])
    ks_copy = pltpu.make_async_copy(ks_hbm, ks_v, local_sem.at[3])
    vs_copy = pltpu.make_async_copy(vs_hbm, vs_v, local_sem.at[4])
    w_copy = pltpu.make_async_copy(w_hbm, w_v, local_sem.at[5])

    def k_copy(b):
        return pltpu.make_async_copy(k_hbm.at[b], k_v.at[b], k_sem.at[b])

    def v_copy(b):
        return pltpu.make_async_copy(v_hbm.at[b], v_v.at[b], v_sem.at[b])

    for copy in (q_copy, ids_copy, cnt_copy, ks_copy, vs_copy):
        copy.start()

    barrier = pltpu.get_barrier_semaphore()

    for _, peer in peers:
        pl.semaphore_signal(barrier, inc=1, device_id={"seq": peer}, device_id_type=MESH)
    for i in range(1, n_head):
        pl.semaphore_signal(
            barrier, inc=1, device_id={"head": (my_head + i) % n_head}, device_id_type=MESH
        )
    for b in range(seqs):
        k_copy(b).start()
        v_copy(b).start()
    w_copy.start()

    def push(src, dst, which, peer, arrival=None):
        pltpu.make_async_remote_copy(
            src_ref=src,
            dst_ref=dst,
            send_sem=send_sem.at[which],
            recv_sem=recv_sem.at[which if arrival is None else arrival],
            device_id={"seq": peer},
            device_id_type=MESH,
        ).start()

    def whole(ref, which, axis, count, arrival=None):
        block = ref.at[pl.ds(0, count)]
        return pltpu.make_async_remote_copy(
            src_ref=block,
            dst_ref=block,
            send_sem=send_sem.at[which],
            recv_sem=recv_sem.at[which if arrival is None else arrival],
            device_id={axis: 0},
            device_id_type=MESH,
        )

    ids_copy.wait()
    cnt_copy.wait()
    first_page = me * pages
    slot_iota = lax.broadcasted_iota(jnp.int32, (kvl, slots), 1)
    for t in range(steps):
        for b in range(seqs):
            counts = [
                jnp.broadcast_to(cnt_v[t, k][:, b : b + 1], (1, slots)) for k in range(kvl)
            ]
            live = slot_iota < jnp.concatenate(counts, axis=0)
            local = jnp.where(live, ids_v[t, b] - first_page, -1)
            idm[pl.ds((t * seqs + b) * kvl, kvl), :] = local.astype(F32)
    by_slot = jnp.transpose(idm[...])
    page_line = lax.broadcasted_iota(jnp.int32, (slots, pages), 1).astype(F32)
    for t in range(steps):
        for b in range(seqs):
            for k in range(kvl):
                r = (t * seqs + b) * kvl + k
                column = jnp.broadcast_to(by_slot[:, r : r + 1], (slots, pages))
                found = jnp.max(jnp.where(column == page_line, 1.0, 0.0), axis=0, keepdims=True)
                for s in range(8 // steps):
                    hits[b * kvl + k, pl.ds(s * steps + t, 1), :] = found

    q_copy.wait()
    pl.semaphore_wait(barrier, n_seq - 1 + n_head - 1)
    for _, peer in peers:
        push(q_all.at[me], q_all.at[me], 0, peer)

    page_of = lax.broadcasted_iota(jnp.int32, (pages, CHUNK), 0) % chunk_pages
    spot_of = lax.broadcasted_iota(jnp.int32, (pages, CHUNK), 1) // page_len
    spread = jnp.where(page_of == spot_of, 1.0, 0.0).astype(BF16)
    chunk_id = lax.broadcasted_iota(jnp.int32, (chunks, 8, pages), 0)
    in_chunk = lax.broadcasted_iota(jnp.int32, (chunks, 8, pages), 2) // chunk_pages == chunk_id

    def expand(entry):
        stacked = jnp.where(in_chunk, jnp.broadcast_to(entry[None], (chunks, 8, pages)), 0.0)
        stacked = stacked.reshape(chunks * 8, pages).astype(BF16)
        return jnp.dot(stacked, spread, preferred_element_type=F32).reshape(chunks, 8, CHUNK)

    log2e = 1.0 / math.log(2.0)
    score_factor = log2e / math.sqrt(hd)

    for bk in range(seqs * kvl):
        bias[bk] = (expand(hits[bk]) - 1.0) * 1e30

    ks_copy.wait()
    vs_copy.wait()

    def scaled(ref, scales, b, k, c):
        lines = []
        for i in range(chunk_pages):
            p = c * chunk_pages + i
            scale = scales[b * (kvl * pages // 128) + (p // 128) * kvl + k, p % 128]
            codes = ref[b, k, pl.ds(p * page_len, page_len), :].astype(F32)
            lines.append((codes * scale).astype(BF16))
        return jnp.concatenate(lines, axis=0)

    @pl.loop(0, seqs)
    def _(b):
        k_copy(b).wait()
        for c in range(chunks):
            for k in range(kvl):
                kt_v[b, c, pl.ds(k * hd, hd), :] = jnp.transpose(scaled(k_v, ks_v, b, k, c))
        v_copy(b).wait()
        for c in range(chunks):
            for k in range(kvl):
                v_v[b, k, pl.ds(c * CHUNK, CHUNK), :] = scaled(v_v, vs_v, b, k, c)

    whole(q_all, 0, "seq", n_seq - 1).wait_recv()
    q_f32[...] = q_all[...].astype(F32).reshape(group * row_count, hd)

    row_line = lax.broadcasted_iota(jnp.int32, (rows, hd), 0)
    lane_line = lax.broadcasted_iota(jnp.int32, (rows, hd), 1)

    def packed_queries(b):
        mine = q_f32[pl.ds(b, rows, stride=seqs), :]
        return jnp.concatenate(
            [jnp.where(row_line // half == k, mine, 0.0) for k in range(kvl)], axis=1
        ).astype(BF16)

    def score_part(b, part, queries, peak):
        for i in range(PART):
            c = part * PART + i
            raw = jnp.dot(queries, kt_v[b, c], preferred_element_type=F32)
            peaks = []
            for r in range(rows // 8):
                mine = raw[r * 8 : r * 8 + 8] * score_factor + bias[b * kvl + r * 8 // half, c]
                s_buf[b % 2, c, pl.ds(r * 8, 8), :] = mine
                peaks.append(jnp.maximum(mine[:, :128], mine[:, 128:]))
            peak = jnp.maximum(peak, jnp.concatenate(peaks, axis=0))
        return peak

    def value_part(b, part, total, acc):
        for i in range(PART):
            c = part * PART + i
            off = c * CHUNK
            weights = []
            sums = []
            for r in range(rows // 16):
                lines = s_buf[b % 2, c, pl.ds(r * 16, 16), :]
                peak = m_buf[b % 2, pl.ds(r * 16, 16), :]
                lower = jnp.exp2(lines[:, :128] - peak)
                upper = jnp.exp2(lines[:, 128:] - peak)
                sums.append(lower + upper)
                weights.append(jnp.concatenate([lower.astype(BF16), upper.astype(BF16)], axis=1))
            values = jnp.concatenate([v_v[b, k, pl.ds(off, CHUNK), :] for k in range(kvl)], axis=1)
            total = total + jnp.concatenate(sums, axis=0)
            acc = acc + jnp.dot(
                jnp.concatenate(weights, axis=0), values, preferred_element_type=F32
            )
        return total, acc

    def set_peak(b, peak):
        peak = jnp.max(peak, axis=1, keepdims=True)
        m_buf[b % 2] = jnp.broadcast_to(peak, (rows, 128))

    low = jnp.full((rows, 128), -2e30, F32)
    first = packed_queries(0)
    peak = low
    for part in range(chunks // PART):
        peak = score_part(0, part, first, peak)
    set_peak(0, peak)
    for b in range(seqs):
        if b + 1 < seqs:
            queries = packed_queries(b + 1)

        peak = low
        if b + 1 < seqs:
            for part in range(chunks // PART):
                peak = score_part(b + 1, part, queries, peak)
        total = jnp.zeros((rows, 128), F32)
        acc = jnp.zeros((rows, kvl * hd), F32)
        for part in range(chunks // PART):
            total, acc = value_part(b, part, total, acc)
        total = jnp.broadcast_to(jnp.sum(total, axis=1, keepdims=True), (rows, 128))
        mine = jnp.concatenate(
            [acc[k * half : (k + 1) * half, k * hd : (k + 1) * hd] for k in range(kvl)], axis=0
        )
        o_f32[pl.ds(b, rows, stride=seqs), :] = mine / total
        level = m_buf[b % 2] + jnp.log(total) * log2e
        here = jnp.where(lane_line == (row_line % steps) * seqs + b, level, 0.0)
        if b == 0:
            a_buf[...] = here
        else:
            a_buf[...] += here
        if b + 1 < seqs:
            set_peak(b + 1, peak)

    stats = a_buf[pl.ds(0, group, stride=steps), :]
    for t in range(1, steps):
        stats = stats + a_buf[pl.ds(t, group, stride=steps), :]
    st_send[...] = stats.reshape(group, 1, 128)
    o_send[...] = o_f32[...].reshape(group, row_count, hd).astype(BF16)
    for _, peer in peers:
        push(st_send.at[peer], st_in.at[me], 1, peer)
        push(o_send.at[peer], o_in.at[me], 2, peer)
    o_in[me] = o_send[me]
    st_in[me] = st_send[me]
    whole(st_in, 1, "seq", n_seq - 1).wait_recv()
    levels = st_in[...].reshape(group, 128)
    share = jnp.exp2(levels - jnp.max(levels, axis=0, keepdims=True))
    share = share / jnp.sum(share, axis=0, keepdims=True)
    by_row = jnp.transpose(share)[:row_count]
    whole(o_in, 2, "seq", n_seq - 1).wait_recv()
    merged = jnp.zeros((row_count, hd), F32)
    for r in range(n_seq):
        merged = merged + by_row[:, r : r + 1] * o_in[r].astype(F32)
    att_all[me] = merged.astype(BF16)
    for step, peer in peers:
        push(att_all.at[me], att_all.at[me], 3, peer, 5 + (planes - step[0]) % planes)

    w_copy.wait()
    partial = None
    for d in sorted(range(planes), key=lambda d: min(d, planes - d)):
        whole(att_all, 3, "seq", plane - (d == 0), 5 + d).wait_recv()
        first_head = plane_first[d]
        flat = jnp.concatenate([att_all[first_head + j] for j in range(plane)], axis=1)
        lines = w_v[pl.ds(pl.multiple_of(first_head * hd, plane * hd), plane * hd), :]
        term = jnp.dot(flat, lines, preferred_element_type=F32)
        partial = term if partial is None else partial + term
    width = partial.shape[1] // n_head
    for h in range(n_head):
        h_send[h] = partial[:, h * width : (h + 1) * width].astype(BF16)
    for i in range(1, n_head):
        peer = (my_head + i) % n_head
        pltpu.make_async_remote_copy(
            src_ref=h_send.at[peer],
            dst_ref=h_in.at[my_head],
            send_sem=send_sem.at[4],
            recv_sem=recv_sem.at[4],
            device_id={"head": peer},
            device_id_type=MESH,
        ).start()
    h_in[my_head] = h_send[my_head]
    for which, ref in ((0, q_all), (1, st_in), (2, o_in), (3, att_all)):
        whole(ref, which, "seq", n_seq - 1).wait_send()
    whole(h_in, 4, "head", n_head - 1).wait_recv()
    whole(h_in, 4, "head", n_head - 1).wait_send()
    summed = h_in[0].astype(F32)
    for h in range(1, n_head):
        summed = summed + h_in[h].astype(F32)
    out_ref[...] = summed.astype(BF16)


def body(
    queries, key_codes, value_codes, key_scales, value_scales, page_ids, page_counts, out_weight,
    *, n_seq, n_head
):
    steps, seqs, _, _, hd = queries.shape
    _, kvl, pages, page_len, _ = key_codes.shape
    row_count = steps * seqs
    group = n_seq
    rows = group * steps
    positions = pages * page_len
    chunks = positions // CHUNK
    columns = out_weight.shape[1]
    slots = page_ids.shape[3]
    width = columns // n_head

    def by_line(scales):
        scales = scales.reshape(seqs, kvl, pages // 128, 128)
        return jnp.transpose(scales, (0, 2, 1, 3)).reshape(-1, 128)

    any_space = pl.BlockSpec(memory_space=pltpu.HBM)
    sizes = (n_seq, n_head, steps, seqs, kvl, pages, page_len, hd)
    out = pl.pallas_call(
        functools.partial(attend_kernel, sizes),
        out_shape=pltpu.VMEM((row_count, width), BF16),
        in_specs=[any_space] * 8,
        out_specs=pl.BlockSpec(memory_space=pltpu.VMEM),
        scratch_shapes=[
            pltpu.VMEM((seqs, kvl, positions, hd), BF16),
            pltpu.VMEM((seqs, kvl, positions, hd), BF16),
            pltpu.VMEM(out_weight.shape, BF16),
            pltpu.SMEM((seqs * kvl * pages // 128, 128), F32),
            pltpu.SMEM((seqs * kvl * pages // 128, 128), F32),
            pltpu.VMEM(page_ids.shape, jnp.int32),
            pltpu.VMEM((steps, kvl, 1, seqs), jnp.int32),
            pltpu.VMEM((seqs, chunks, kvl * hd, CHUNK), BF16),
            pltpu.VMEM((steps * seqs * kvl, slots), F32),
            pltpu.VMEM((seqs * kvl, 8, pages), F32),
            pltpu.VMEM((seqs * kvl, chunks, 8, CHUNK), F32),
            pltpu.VMEM((group, row_count, hd), BF16),
            pltpu.VMEM((group * row_count, hd), F32),
            pltpu.VMEM((2, chunks, rows, CHUNK), F32),
            pltpu.VMEM((2, rows, 128), F32),
            pltpu.VMEM((group * row_count, hd), F32),
            pltpu.VMEM((rows, 128), F32),
            pltpu.VMEM((group, row_count, hd), BF16),
            pltpu.VMEM((group, row_count, hd), BF16),
            pltpu.VMEM((group, 1, 128), F32),
            pltpu.VMEM((group, 1, 128), F32),
            pltpu.VMEM((group, row_count, hd), BF16),
            pltpu.VMEM((n_head, row_count, width), BF16),
            pltpu.VMEM((n_head, row_count, width), BF16),
            pltpu.SemaphoreType.DMA((6,)),
            pltpu.SemaphoreType.DMA((seqs,)),
            pltpu.SemaphoreType.DMA((seqs,)),
            pltpu.SemaphoreType.DMA((5,)),
            pltpu.SemaphoreType.DMA((9,)),
        ],
        compiler_params=pltpu.CompilerParams(
            collective_id=0, has_side_effects=True, vmem_limit_bytes=60 * 1024 * 1024
        ),
        name="attend",
    )(
        queries.reshape(row_count, hd),
        key_codes.reshape(seqs, kvl, positions, hd),
        value_codes.reshape(seqs, kvl, positions, hd),
        by_line(key_scales),
        by_line(value_scales),
        page_ids,
        jnp.transpose(page_counts, (0, 2, 3, 1)),
        out_weight,
    )
    return out.reshape(steps, seqs, width)


def solution(mesh):
    placed = (
        P(None, None, "head", "seq", None),
        P(None, "head", "seq", None, None),
        P(None, "head", "seq", None, None),
        P(None, "head", "seq"),
        P(None, "head", "seq"),
        P(None, None, "head", "seq"),
        P(None, None, "head", "seq"),
        P("head", "seq"),
    )
    step = functools.partial(body, n_seq=mesh.shape["seq"], n_head=mesh.shape["head"])
    return jax.shard_map(
        step, mesh=mesh, in_specs=placed, out_specs=P(None, None, ("seq", "head")), check_vma=False
    )
```

```python
import functools
import math

import jax
import jax.numpy as jnp
from jax import lax
from jax.experimental import pallas as pl
from jax.experimental.pallas import tpu as pltpu
from jax.sharding import PartitionSpec as P

MESH = pl.DeviceIdType.MESH
F32 = jnp.float32
BF16 = jnp.bfloat16
CHUNK = 256
PART = 4


def seq_offsets(count):
    parts = (4, 4, 2) if count == 32 else (1, 1, count)
    steps = [(i, j, k) for i in range(parts[0]) for j in range(parts[1]) for k in range(parts[2])]
    ring = lambda d, n: min(d, n - d)
    steps = sorted(steps, key=lambda o: -(4 * (ring(o[0], parts[0]) + ring(o[1], parts[1])) + o[2]))
    return parts, steps[:-1]


def seq_peers(me, count):
    parts, steps = seq_offsets(count)
    x, z, core = me // (parts[1] * parts[2]), (me // parts[2]) % parts[1], me % parts[2]
    xs = [((x + d) % parts[0]) * (parts[1] * parts[2]) for d in range(parts[0])]
    zs = [((z + d) % parts[1]) * parts[2] for d in range(parts[1])]
    cores = [(core + d) % parts[2] for d in range(parts[2])]
    return [(o, xs[o[0]] + zs[o[1]] + cores[o[2]]) for o in steps], parts, xs


def attend_kernel(
    sizes,
    q_hbm,
    k_hbm,
    v_hbm,
    ks_hbm,
    vs_hbm,
    ids_hbm,
    cnt_hbm,
    w_hbm,
    out_ref,
    k_v,
    v_v,
    w_v,
    ks_v,
    vs_v,
    ids_v,
    cnt_v,
    kt_v,
    idm,
    hits,
    bias,
    q_all,
    q_f32,
    s_buf,
    m_buf,
    o_f32,
    a_buf,
    o_send,
    o_in,
    st_send,
    st_in,
    att_all,
    h_send,
    h_in,
    local_sem,
    k_sem,
    v_sem,
    send_sem,
    recv_sem,
):
    n_seq, n_head, steps, seqs, kvl, pages, page_len, hd = sizes
    group = n_seq
    rows = group * steps
    half = rows // kvl
    positions = pages * page_len
    chunks = positions // CHUNK
    chunk_pages = CHUNK // page_len
    slots = ids_v.shape[3]
    row_count = steps * seqs
    me = lax.axis_index("seq")
    my_head = lax.axis_index("head")
    peers, parts, plane_first = seq_peers(me, n_seq)
    planes = parts[0]
    plane = n_seq // planes

    q_copy = pltpu.make_async_copy(q_hbm, q_all.at[me], local_sem.at[0])
    ids_copy = pltpu.make_async_copy(ids_hbm, ids_v, local_sem.at[1])
    cnt_copy = pltpu.make_async_copy(cnt_hbm, cnt_v, local_sem.at[2])
    ks_copy = pltpu.make_async_copy(ks_hbm, ks_v, local_sem.at[3])
    vs_copy = pltpu.make_async_copy(vs_hbm, vs_v, local_sem.at[4])
    w_copy = pltpu.make_async_copy(w_hbm, w_v, local_sem.at[5])

    def k_copy(b):
        return pltpu.make_async_copy(k_hbm.at[b], k_v.at[b], k_sem.at[b])

    def v_copy(b):
        return pltpu.make_async_copy(v_hbm.at[b], v_v.at[b], v_sem.at[b])

    for copy in (q_copy, ids_copy, cnt_copy, ks_copy, vs_copy):
        copy.start()

    barrier = pltpu.get_barrier_semaphore()

    for _, peer in peers:
        pl.semaphore_signal(barrier, inc=1, device_id={"seq": peer}, device_id_type=MESH)
    for i in range(1, n_head):
        pl.semaphore_signal(
            barrier, inc=1, device_id={"head": (my_head + i) % n_head}, device_id_type=MESH
        )
    for b in range(seqs):
        k_copy(b).start()
        v_copy(b).start()
    w_copy.start()

    def push(src, dst, which, peer, arrival=None):
        pltpu.make_async_remote_copy(
            src_ref=src,
            dst_ref=dst,
            send_sem=send_sem.at[which],
            recv_sem=recv_sem.at[which if arrival is None else arrival],
            device_id={"seq": peer},
            device_id_type=MESH,
        ).start()

    def whole(ref, which, axis, count, arrival=None):
        block = ref.at[pl.ds(0, count)]
        return pltpu.make_async_remote_copy(
            src_ref=block,
            dst_ref=block,
            send_sem=send_sem.at[which],
            recv_sem=recv_sem.at[which if arrival is None else arrival],
            device_id={axis: 0},
            device_id_type=MESH,
        )

    ids_copy.wait()
    cnt_copy.wait()
    first_page = me * pages
    slot_iota = lax.broadcasted_iota(jnp.int32, (kvl, slots), 1)
    for t in range(steps):
        for b in range(seqs):
            counts = [
                jnp.broadcast_to(cnt_v[t, k][:, b : b + 1], (1, slots)) for k in range(kvl)
            ]
            live = slot_iota < jnp.concatenate(counts, axis=0)
            local = jnp.where(live, ids_v[t, b] - first_page, -1)
            idm[pl.ds((t * seqs + b) * kvl, kvl), :] = local.astype(F32)
    by_slot = jnp.transpose(idm[...])
    page_line = lax.broadcasted_iota(jnp.int32, (slots, pages), 1).astype(F32)
    for t in range(steps):
        for b in range(seqs):
            for k in range(kvl):
                r = (t * seqs + b) * kvl + k
                column = jnp.broadcast_to(by_slot[:, r : r + 1], (slots, pages))
                found = jnp.max(jnp.where(column == page_line, 1.0, 0.0), axis=0, keepdims=True)
                for s in range(8 // steps):
                    hits[b * kvl + k, pl.ds(s * steps + t, 1), :] = found

    page_of = lax.broadcasted_iota(jnp.int32, (pages, CHUNK), 0) % chunk_pages
    spot_of = lax.broadcasted_iota(jnp.int32, (pages, CHUNK), 1) // page_len
    spread = jnp.where(page_of == spot_of, 1.0, 0.0).astype(BF16)
    chunk_id = lax.broadcasted_iota(jnp.int32, (chunks, 8, pages), 0)
    in_chunk = lax.broadcasted_iota(jnp.int32, (chunks, 8, pages), 2) // chunk_pages == chunk_id

    def expand(entry):
        stacked = jnp.where(in_chunk, jnp.broadcast_to(entry[None], (chunks, 8, pages)), 0.0)
        stacked = stacked.reshape(chunks * 8, pages).astype(BF16)
        return jnp.dot(stacked, spread, preferred_element_type=F32).reshape(chunks, 8, CHUNK)

    log2e = 1.0 / math.log(2.0)
    score_factor = log2e / math.sqrt(hd)

    for bk in range(seqs * kvl):
        bias[bk] = (expand(hits[bk]) - 1.0) * 1e30

    q_copy.wait()
    pl.semaphore_wait(barrier, n_seq - 1 + n_head - 1)
    for _, peer in peers:
        push(q_all.at[me], q_all.at[me], 0, peer)

    ks_copy.wait()
    vs_copy.wait()

    def scaled(ref, scales, b, k, c):
        lines = []
        for i in range(chunk_pages):
            p = c * chunk_pages + i
            scale = scales[b * (kvl * pages // 128) + (p // 128) * kvl + k, p % 128]
            codes = ref[b, k, pl.ds(p * page_len, page_len), :].astype(F32)
            lines.append((codes * scale).astype(BF16))
        return jnp.concatenate(lines, axis=0)

    @pl.loop(0, seqs)
    def _(b):
        k_copy(b).wait()
        for c in range(chunks):
            for k in range(kvl):
                kt_v[b, c, pl.ds(k * hd, hd), :] = jnp.transpose(scaled(k_v, ks_v, b, k, c))
        v_copy(b).wait()
        for c in range(chunks):
            for k in range(kvl):
                v_v[b, k, pl.ds(c * CHUNK, CHUNK), :] = scaled(v_v, vs_v, b, k, c)

    whole(q_all, 0, "seq", n_seq - 1).wait_recv()
    q_f32[...] = q_all[...].astype(F32).reshape(group * row_count, hd)

    row_line = lax.broadcasted_iota(jnp.int32, (rows, hd), 0)
    lane_line = lax.broadcasted_iota(jnp.int32, (rows, hd), 1)

    def packed_queries(b):
        mine = q_f32[pl.ds(b, rows, stride=seqs), :]
        return jnp.concatenate(
            [jnp.where(row_line // half == k, mine, 0.0) for k in range(kvl)], axis=1
        ).astype(BF16)

    def score_part(b, part, queries, peak):
        for i in range(PART):
            c = part * PART + i
            raw = jnp.dot(queries, kt_v[b, c], preferred_element_type=F32)
            peaks = []
            for r in range(rows // 8):
                mine = raw[r * 8 : r * 8 + 8] * score_factor + bias[b * kvl + r * 8 // half, c]
                s_buf[b % 2, c, pl.ds(r * 8, 8), :] = mine
                peaks.append(jnp.maximum(mine[:, :128], mine[:, 128:]))
            peak = jnp.maximum(peak, jnp.concatenate(peaks, axis=0))
        return peak

    def value_part(b, part, total, acc):
        for i in range(PART):
            c = part * PART + i
            off = c * CHUNK
            weights = []
            sums = []
            for r in range(rows // 16):
                lines = s_buf[b % 2, c, pl.ds(r * 16, 16), :]
                peak = m_buf[b % 2, pl.ds(r * 16, 16), :]
                lower = jnp.exp2(lines[:, :128] - peak)
                upper = jnp.exp2(lines[:, 128:] - peak)
                sums.append(lower + upper)
                weights.append(jnp.concatenate([lower.astype(BF16), upper.astype(BF16)], axis=1))
            values = jnp.concatenate([v_v[b, k, pl.ds(off, CHUNK), :] for k in range(kvl)], axis=1)
            total = total + jnp.concatenate(sums, axis=0)
            acc = acc + jnp.dot(
                jnp.concatenate(weights, axis=0), values, preferred_element_type=F32
            )
        return total, acc

    def set_peak(b, peak):
        peak = jnp.max(peak, axis=1, keepdims=True)
        m_buf[b % 2] = jnp.broadcast_to(peak, (rows, 128))

    low = jnp.full((rows, 128), -2e30, F32)
    first = packed_queries(0)
    peak = low
    for part in range(chunks // PART):
        peak = score_part(0, part, first, peak)
    set_peak(0, peak)
    for b in range(seqs):
        if b + 1 < seqs:
            queries = packed_queries(b + 1)

        peak = low
        if b + 1 < seqs:
            for part in range(chunks // PART):
                peak = score_part(b + 1, part, queries, peak)
        total = jnp.zeros((rows, 128), F32)
        acc = jnp.zeros((rows, kvl * hd), F32)
        for part in range(chunks // PART):
            total, acc = value_part(b, part, total, acc)
        total = jnp.broadcast_to(jnp.sum(total, axis=1, keepdims=True), (rows, 128))
        mine = jnp.concatenate(
            [acc[k * half : (k + 1) * half, k * hd : (k + 1) * hd] for k in range(kvl)], axis=0
        )
        o_f32[pl.ds(b, rows, stride=seqs), :] = mine / total
        level = m_buf[b % 2] + jnp.log(total) * log2e
        here = jnp.where(lane_line == (row_line % steps) * seqs + b, level, 0.0)
        if b == 0:
            a_buf[...] = here
        else:
            a_buf[...] += here
        if b + 1 < seqs:
            set_peak(b + 1, peak)

    stats = a_buf[pl.ds(0, group, stride=steps), :]
    for t in range(1, steps):
        stats = stats + a_buf[pl.ds(t, group, stride=steps), :]
    st_send[...] = stats.reshape(group, 1, 128)
    o_send[...] = o_f32[...].reshape(group, row_count, hd).astype(BF16)
    for _, peer in peers:
        push(st_send.at[peer], st_in.at[me], 1, peer)
        push(o_send.at[peer], o_in.at[me], 2, peer)
    o_in[me] = o_send[me]
    st_in[me] = st_send[me]
    whole(st_in, 1, "seq", n_seq - 1).wait_recv()
    levels = st_in[...].reshape(group, 128)
    share = jnp.exp2(levels - jnp.max(levels, axis=0, keepdims=True))
    share = share / jnp.sum(share, axis=0, keepdims=True)
    by_row = jnp.transpose(share)[:row_count]
    whole(o_in, 2, "seq", n_seq - 1).wait_recv()
    merged = jnp.zeros((row_count, hd), F32)
    for r in range(n_seq):
        merged = merged + by_row[:, r : r + 1] * o_in[r].astype(F32)
    att_all[me] = merged.astype(BF16)
    for step, peer in peers:
        push(att_all.at[me], att_all.at[me], 3, peer, 5 + (planes - step[0]) % planes)

    w_copy.wait()
    partial = None
    for d in sorted(range(planes), key=lambda d: min(d, planes - d)):
        whole(att_all, 3, "seq", plane - (d == 0), 5 + d).wait_recv()
        first_head = plane_first[d]
        flat = jnp.concatenate([att_all[first_head + j] for j in range(plane)], axis=1)
        lines = w_v[pl.ds(pl.multiple_of(first_head * hd, plane * hd), plane * hd), :]
        term = jnp.dot(flat, lines, preferred_element_type=F32)
        partial = term if partial is None else partial + term
    width = partial.shape[1] // n_head
    for h in range(n_head):
        h_send[h] = partial[:, h * width : (h + 1) * width].astype(BF16)
    for i in range(1, n_head):
        peer = (my_head + i) % n_head
        pltpu.make_async_remote_copy(
            src_ref=h_send.at[peer],
            dst_ref=h_in.at[my_head],
            send_sem=send_sem.at[4],
            recv_sem=recv_sem.at[4],
            device_id={"head": peer},
            device_id_type=MESH,
        ).start()
    h_in[my_head] = h_send[my_head]
    for which, ref in ((0, q_all), (1, st_in), (2, o_in), (3, att_all)):
        whole(ref, which, "seq", n_seq - 1).wait_send()
    whole(h_in, 4, "head", n_head - 1).wait_recv()
    whole(h_in, 4, "head", n_head - 1).wait_send()
    summed = h_in[0].astype(F32)
    for h in range(1, n_head):
        summed = summed + h_in[h].astype(F32)
    out_ref[...] = summed.astype(BF16)


def body(
    queries, key_codes, value_codes, key_scales, value_scales, page_ids, page_counts, out_weight,
    *, n_seq, n_head
):
    steps, seqs, _, _, hd = queries.shape
    _, kvl, pages, page_len, _ = key_codes.shape
    row_count = steps * seqs
    group = n_seq
    rows = group * steps
    positions = pages * page_len
    chunks = positions // CHUNK
    columns = out_weight.shape[1]
    slots = page_ids.shape[3]
    width = columns // n_head

    def by_line(scales):
        scales = scales.reshape(seqs, kvl, pages // 128, 128)
        return jnp.transpose(scales, (0, 2, 1, 3)).reshape(-1, 128)

    any_space = pl.BlockSpec(memory_space=pltpu.HBM)
    sizes = (n_seq, n_head, steps, seqs, kvl, pages, page_len, hd)
    out = pl.pallas_call(
        functools.partial(attend_kernel, sizes),
        out_shape=pltpu.VMEM((row_count, width), BF16),
        in_specs=[any_space] * 8,
        out_specs=pl.BlockSpec(memory_space=pltpu.VMEM),
        scratch_shapes=[
            pltpu.VMEM((seqs, kvl, positions, hd), BF16),
            pltpu.VMEM((seqs, kvl, positions, hd), BF16),
            pltpu.VMEM(out_weight.shape, BF16),
            pltpu.SMEM((seqs * kvl * pages // 128, 128), F32),
            pltpu.SMEM((seqs * kvl * pages // 128, 128), F32),
            pltpu.VMEM(page_ids.shape, jnp.int32),
            pltpu.VMEM((steps, kvl, 1, seqs), jnp.int32),
            pltpu.VMEM((seqs, chunks, kvl * hd, CHUNK), BF16),
            pltpu.VMEM((steps * seqs * kvl, slots), F32),
            pltpu.VMEM((seqs * kvl, 8, pages), F32),
            pltpu.VMEM((seqs * kvl, chunks, 8, CHUNK), F32),
            pltpu.VMEM((group, row_count, hd), BF16),
            pltpu.VMEM((group * row_count, hd), F32),
            pltpu.VMEM((2, chunks, rows, CHUNK), F32),
            pltpu.VMEM((2, rows, 128), F32),
            pltpu.VMEM((group * row_count, hd), F32),
            pltpu.VMEM((rows, 128), F32),
            pltpu.VMEM((group, row_count, hd), BF16),
            pltpu.VMEM((group, row_count, hd), BF16),
            pltpu.VMEM((group, 1, 128), F32),
            pltpu.VMEM((group, 1, 128), F32),
            pltpu.VMEM((group, row_count, hd), BF16),
            pltpu.VMEM((n_head, row_count, width), BF16),
            pltpu.VMEM((n_head, row_count, width), BF16),
            pltpu.SemaphoreType.DMA((6,)),
            pltpu.SemaphoreType.DMA((seqs,)),
            pltpu.SemaphoreType.DMA((seqs,)),
            pltpu.SemaphoreType.DMA((5,)),
            pltpu.SemaphoreType.DMA((9,)),
        ],
        compiler_params=pltpu.CompilerParams(
            collective_id=0, has_side_effects=True, vmem_limit_bytes=60 * 1024 * 1024
        ),
        name="attend",
    )(
        queries.reshape(row_count, hd),
        key_codes.reshape(seqs, kvl, positions, hd),
        value_codes.reshape(seqs, kvl, positions, hd),
        by_line(key_scales),
        by_line(value_scales),
        page_ids,
        jnp.transpose(page_counts, (0, 2, 3, 1)),
        out_weight,
    )
    return out.reshape(steps, seqs, width)


def solution(mesh):
    placed = (
        P(None, None, "head", "seq", None),
        P(None, "head", "seq", None, None),
        P(None, "head", "seq", None, None),
        P(None, "head", "seq"),
        P(None, "head", "seq"),
        P(None, None, "head", "seq"),
        P(None, None, "head", "seq"),
        P("head", "seq"),
    )
    step = functools.partial(body, n_seq=mesh.shape["seq"], n_head=mesh.shape["head"])
    return jax.shard_map(
        step, mesh=mesh, in_specs=placed, out_specs=P(None, None, ("seq", "head")), check_vma=False
    )
```
